32 devices in a mesh: leaf: 16 (over z, y, x), sep: 2 (over core).
Axes of the slice: x: 2, y: 2, z: 4, core: 2. Of those that a mesh axis runs over, the one named last changes fastest.
Arguments:
- leaf_rhs: bfloat16 [16, 256, 2048], P('leaf', None, 'sep'), may hold values from -6 to 6
- leaf_inv: bfloat16 [16, 2048, 2048], P('leaf', 'sep'), may hold values from -0.125 to 0.125
- leaf_couple: bfloat16 [16, 512, 2048], P('leaf', None, 'sep'), may hold values from -0.0625 to 0.0625
- sep_rhs: float32 [16, 256, 512], P('leaf', None, 'sep'), may hold values from -6 to 6
- sep_inv: float32 [16, 512, 512], P('leaf', 'sep'), may hold values from -0.25 to 0.25
- sep_couple: float32 [16, 512, 512], P('leaf', None, 'sep'), may hold values from -0.1875 to 0.1875
Outputs:
- leaf_solution: float32 [16, 256, 2048], P('leaf', None, 'sep')
- sep_solution: float32 [16, 256, 512], P('leaf', None, 'sep')
The draws below stay inside these ranges and needn't reach their ends.
All inputs are finite; a program needn't handle non-finite values.
Results may differ from the reference program's by a relative error of at most 0.0042.
Values may be sent and summed in bfloat16 or wider, within the bound.
No kernel may reach another device: no remote copies, remote signals or barrier semaphores. Data moves between devices by JAX's collectives and lax.ppermute only.
A program may use at most 128 MiB of HBM per device.

```python
import jax
import jax.numpy as jnp
import numpy as np
from jax import lax

NI = 2048
S = 512
RHS = 256
LEAVES = 16
LEVELS = 4


def levels(key, extent, shards, smallest, high):
    factor_of = 1.0
    for axis_at, parts in shards:
        steps = jax.random.uniform(jax.random.fold_in(jax.random.fold_in(key, 6), axis_at), (parts,), jnp.float32, smallest / len(shards), high / len(shards))
        factor_of = factor_of * jnp.repeat(jnp.exp(steps), extent[axis_at] // parts).reshape((-1,) + (1,) * (len(extent) - 1 - axis_at))
    return factor_of


def gaussian(key, shape, deviation, most, shards=(), held_as=jnp.bfloat16):
    result = jax.random.normal(key, shape, jnp.float32) * deviation
    if len(shards) > 0:
        result = levels(key, shape, shards, -0.22, 0.18) * result
    return jnp.clip(result, min=-most, max=most).astype(held_as)


def setup_inputs(seed: int = 0) -> dict:
    arg_keys = jax.random.split(jax.random.key(seed), 7)
    return {
        "leaf_rhs": gaussian(arg_keys[0], (LEAVES, RHS, NI), 1.0, 6.0, ((0, 16), (2, 2))),
        "leaf_inv": gaussian(arg_keys[1], (LEAVES, NI, NI), NI ** -0.5, 0.125, ((0, 16), (1, 2))),
        "leaf_couple": gaussian(arg_keys[2], (LEAVES, S, NI), (4 * NI) ** -0.5, 0.0625, ((0, 16), (2, 2))),
        "sep_rhs": gaussian(arg_keys[3], (LEAVES, RHS, S), 1.0, 6.0, ((0, 16), (2, 2)), jnp.float32),
        "sep_inv": gaussian(arg_keys[4], (LEAVES, S, S), S ** -0.5, 0.25, ((0, 16), (1, 2)), jnp.float32),
        "sep_couple": gaussian(arg_keys[5], (LEAVES, S, S), (2 * S) ** -0.5, 0.1875, ((0, 16), (2, 2)), jnp.float32),
    }


def leaf_up(items):
    rhs, inverse, couple = items
    dims = (((1,), (1,)), ((), ()))
    state = lax.dot_general(rhs, inverse, dims, preferred_element_type=jnp.float32).astype(jnp.bfloat16)
    return state, lax.dot_general(state, couple, dims, preferred_element_type=jnp.float32)


def leaf_down(items):
    state, parent, couple, inverse = items
    pulled = jnp.dot(parent.astype(jnp.bfloat16), couple, preferred_element_type=jnp.float32)
    residue = (state.astype(jnp.float32) - pulled).astype(jnp.bfloat16)
    return jnp.dot(residue, inverse, preferred_element_type=jnp.float32)


def reference(leaf_rhs, leaf_inv, leaf_couple, sep_rhs, sep_inv, sep_couple):
    count = leaf_rhs.shape[0]
    high = lax.Precision.HIGHEST
    leaf_state, leaf_out = lax.map(leaf_up, (leaf_rhs, leaf_inv, leaf_couple))
    sep_state = jnp.zeros(sep_rhs.shape, jnp.float32)
    outgoing = leaf_out
    for section in range(1, LEVELS + 2):
        slots = np.arange(2 ** (section - 1) - 1, count, 2 ** section)
        if section == 1:
            children = outgoing[slots] + outgoing[slots + 1]
        elif section <= LEVELS:
            reach = 2 ** (section - 2)
            children = outgoing[slots - reach] + outgoing[slots + reach]
        else:
            children = outgoing[slots - 2 ** (section - 2)]
        work = sep_rhs[slots] - children
        fresh = jnp.einsum("brk,bmk->brm", work, sep_inv[slots], precision=high)
        sep_state = sep_state.at[slots].set(fresh)
        if section <= LEVELS:
            sent = jnp.einsum("brk,bmk->brm", fresh, sep_couple[slots], precision=high)
            outgoing = jnp.zeros(sep_rhs.shape, jnp.float32).at[slots].set(sent)
    sep_solution = jnp.zeros(sep_rhs.shape, jnp.float32)
    for section in range(LEVELS + 1, 0, -1):
        slots = np.arange(2 ** (section - 1) - 1, count, 2 ** section)
        if section == LEVELS + 1:
            work = sep_state[slots]
        else:
            reach = 2 ** (section - 1)
            parent = np.where(((slots >> section) & 1) == 0, slots + reach, slots - reach)
            work = sep_state[slots] - jnp.einsum("brk,bkm->brm", sep_solution[parent], sep_couple[slots], precision=high)
        solved = jnp.einsum("brk,bkm->brm", work, sep_inv[slots], precision=high)
        sep_solution = sep_solution.at[slots].set(solved)
    numbers = np.arange(count)
    parents = numbers - numbers % 2
    leaf_solution = lax.map(leaf_down, (leaf_state, sep_solution[parents], leaf_couple, leaf_inv))
    return leaf_solution, sep_solution
```

```python
import jax
import jax.numpy as jnp
from jax import lax
from jax.sharding import PartitionSpec as P

ROWS = (((1,), (0,)), ((), ()))
BOTH = (((1,), (1,)), ((), ()))
FIRST = (((0,), (0,)), ((), ()))


def product(left, right, dims, precision=lax.Precision.HIGH):
    return lax.dot_general(
        left, right, dims, precision=precision, preferred_element_type=jnp.float32
    )


def swap(value):
    pairs = [(source, source ^ 1) for source in range(lax.axis_size("sep"))]
    return lax.ppermute(value, "sep", pairs)


def send(value, pairs):
    return lax.ppermute(value.astype(jnp.bfloat16), "leaf", pairs).astype(jnp.float32)


def join(mine, other, first, axis):
    return jnp.where(
        first,
        jnp.concatenate([mine, other], axis=axis),
        jnp.concatenate([other, mine], axis=axis),
    )


def local(leaf_rhs, leaf_inv, leaf_couple, sep_rhs, sep_inv, sep_couple):
    count = lax.axis_size("leaf")
    depth = count.bit_length() - 1
    place = lax.axis_index("leaf")
    core = lax.axis_index("sep")
    first = core == 0
    even = place % 2 == 0
    inv_rows = leaf_inv[0]
    couple_cols = leaf_couple[0]
    half = leaf_rhs.shape[1] // 2
    half_sep = sep_rhs.shape[2]
    top, below = count - 1, count // 2 - 1

    def my_rows(value):
        return lax.dynamic_slice_in_dim(value, core * half, half, 0)

    def other_rows(value):
        return lax.dynamic_slice_in_dim(value, (1 - core) * half, half, 0)

    rhs_full = join(leaf_rhs[0], swap(leaf_rhs[0]), first, 1)
    leaf_state = lax.dot_general(
        rhs_full, inv_rows, BOTH, preferred_element_type=jnp.float32
    ).astype(jnp.bfloat16)
    theirs = product(other_rows(leaf_state), couple_cols, BOTH, None)
    ours = product(my_rows(leaf_state), couple_cols, BOTH, None)

    sep_local = sep_rhs[0]
    rhs_rows = join(my_rows(sep_local), swap(other_rows(sep_local)), first, 1)
    inv_half = sep_inv[0]
    inverse = join(inv_half, swap(inv_half), first, 0)
    couple = join(sep_couple[0], swap(sep_couple[0]), first, 1)
    pull = product(couple, inverse, ROWS, lax.Precision.HIGHEST)
    gram = product(inverse, inverse, FIRST, lax.Precision.HIGHEST)
    top_rhs = lax.ppermute(rhs_rows, "leaf", [(top, below)])
    top_half = lax.ppermute(inv_half, "leaf", [(top, below)])
    top_inverse = join(top_half, swap(top_half), first, 0)
    top_gram = product(top_inverse, top_inverse, FIRST, lax.Precision.HIGHEST)

    outgoing = ours + swap(theirs)
    work = rhs_rows - jnp.where(even, outgoing, 0.0)
    work = work - send(outgoing, [(k + 1, k) for k in range(0, count, 2)])
    for level in range(1, depth):
        reach = 2 ** (level - 1)
        parents = range(2 * reach - 1, count, 4 * reach)
        outgoing = product(work, pull, BOTH)
        lower = send(outgoing, [(k - reach, k) for k in parents])
        upper = send(outgoing, [(k + reach, k) for k in parents])
        work = work - (lower + upper)
    top_work = top_rhs - product(work, pull, BOTH)
    top_solution = product(top_work, top_gram, ROWS)
    parent = top_solution
    state = product(work, gram, ROWS)
    for level in range(depth, 1, -1):
        reach = 2 ** (level - 2)
        slots = range(2 * reach - 1, count, 4 * reach)
        solved = state - product(parent, pull, ROWS)
        lower = send(solved, [(k, k - reach) for k in slots])
        upper = send(solved, [(k, k + reach) for k in slots])
        parent = parent + (lower + upper)
    solved = state - product(parent, pull, ROWS)
    beside = lax.ppermute(
        solved.astype(jnp.bfloat16), "leaf", [(k, k + 1) for k in range(0, count, 2)]
    )
    parent_rows = jnp.where(even, solved.astype(jnp.bfloat16), beside)

    parent_full = join(parent_rows, swap(parent_rows), first, 0)
    pulled = jnp.dot(parent_full, couple_cols, preferred_element_type=jnp.float32)
    residue = (leaf_state.astype(jnp.float32) - pulled).astype(jnp.bfloat16)
    spread = jnp.dot(residue, inv_rows, preferred_element_type=jnp.float32)
    wide = leaf_rhs.shape[2]
    away = lax.dynamic_slice_in_dim(spread, (1 - core) * wide, wide, 1)
    here = lax.dynamic_slice_in_dim(spread, core * wide, wide, 1)
    leaf_solution = here + swap(away)

    from_below = lax.ppermute(top_solution, "leaf", [(below, top)])
    whole = jnp.where(place == top, from_below, solved)
    away = lax.dynamic_slice_in_dim(whole, (1 - core) * half_sep, half_sep, 1)
    here = lax.dynamic_slice_in_dim(whole, core * half_sep, half_sep, 1)
    sep_solution = join(here, swap(away), first, 0)
    return (leaf_solution[None], sep_solution[None])


def solution(mesh):
    return jax.shard_map(
        local,
        mesh=mesh,
        in_specs=(
            P("leaf", None, "sep"),
            P("leaf", "sep", None),
            P("leaf", None, "sep"),
            P("leaf", None, "sep"),
            P("leaf", "sep", None),
            P("leaf", None, "sep"),
        ),
        out_specs=(P("leaf", None, "sep"), P("leaf", None, "sep")),
        check_vma=False,
    )
```

```python
import jax
import jax.numpy as jnp
from jax import lax
from jax.sharding import PartitionSpec as P


ROWS = (((1,), (0,)), ((), ()))
BOTH = (((1,), (1,)), ((), ()))
FIRST = (((0,), (0,)), ((), ()))


def product(left, right, dims, precision=lax.Precision.HIGH):
    return lax.dot_general(
        left, right, dims, precision=precision, preferred_element_type=jnp.float32
    )


def swap(value):
    pairs = [(source, source ^ 1) for source in range(lax.axis_size("sep"))]
    return lax.ppermute(value, "sep", pairs)


def send(value, pairs):
    return lax.ppermute(value.astype(jnp.bfloat16), "leaf", pairs).astype(jnp.float32)


def join(mine, other, first, axis):
    return jnp.where(
        first,
        jnp.concatenate([mine, other], axis=axis),
        jnp.concatenate([other, mine], axis=axis),
    )


def columns(value, which, wide):
    return lax.dynamic_slice_in_dim(value, which * wide, wide, 1)


def solve(leaf_rhs, leaf_inv, leaf_couple, sep_rhs, sep_inv, sep_couple):
    count = lax.axis_size("leaf")
    depth = count.bit_length() - 1
    place = lax.axis_index("leaf")
    core = lax.axis_index("sep")
    first = core == 0
    even = place % 2 == 0
    inv_rows = leaf_inv[0]
    couple_cols = leaf_couple[0]
    half = leaf_rhs.shape[1] // 2
    half_sep = sep_rhs.shape[2]
    top, below = count - 1, count // 2 - 1

    def my_rows(value):
        return lax.dynamic_slice_in_dim(value, core * half, half, 0)

    def other_rows(value):
        return lax.dynamic_slice_in_dim(value, (1 - core) * half, half, 0)

    wide = leaf_rhs.shape[2]
    inv_half, couple_half, sep_local = sep_inv[0], sep_couple[0], sep_rhs[0]
    rhs_own = leaf_rhs[0]
    rhs_other = swap(rhs_own)
    top_half = lax.ppermute(inv_half, "leaf", [(top, below)])
    near = product(rhs_own, columns(inv_rows, core, wide), BOTH, None)
    far = product(rhs_other, columns(inv_rows, 1 - core, wide), BOTH, None)
    leaf_state = (near + far).astype(jnp.bfloat16)
    theirs = product(other_rows(leaf_state), couple_cols, BOTH, None)
    ours = product(my_rows(leaf_state), couple_cols, BOTH, None)

    rhs_rows = join(my_rows(sep_local), swap(other_rows(sep_local)), first, 1)

    def both_cores(part):
        return part + swap(part)

    outgoing = ours + swap(theirs)
    couple_late, inv_late, _ = lax.optimization_barrier((couple_half, inv_half, leaf_state))
    pull = both_cores(product(couple_late, inv_late, ROWS))
    work = rhs_rows - jnp.where(even, outgoing, 0.0)
    work = work - send(outgoing, [(k + 1, k) for k in range(0, count, 2)])
    for level in range(1, depth):
        reach = 2 ** (level - 1)
        parents = range(2 * reach - 1, count, 4 * reach)
        outgoing = product(work, pull, BOTH)
        lower = send(outgoing, [(k - reach, k) for k in parents])
        upper = send(outgoing, [(k + reach, k) for k in parents])
        if level == 1:
            inv_late, rhs_late, _ = lax.optimization_barrier((inv_half, rhs_rows, outgoing))
            gram = both_cores(product(inv_late, inv_late, FIRST))
            top_rhs = lax.ppermute(rhs_late, "leaf", [(top, below)])
        if level == 2:
            top_late, _ = lax.optimization_barrier((top_half, outgoing))
            top_gram = both_cores(product(top_late, top_late, FIRST))
        work = work - (lower + upper)
    top_work = top_rhs - product(work, pull, BOTH)
    top_solution = product(top_work, top_gram, ROWS)
    parent = top_solution
    state = product(work, gram, ROWS)
    for level in range(depth, 1, -1):
        reach = 2 ** (level - 2)
        slots = range(2 * reach - 1, count, 4 * reach)
        solved = state - product(parent, pull, ROWS)
        lower = send(solved, [(k, k - reach) for k in slots])
        upper = send(solved, [(k, k + reach) for k in slots])
        if level == 2:
            top_late, _ = lax.optimization_barrier((top_solution, solved))
            from_below = lax.ppermute(top_late, "leaf", [(below, top)])
        parent = parent + (lower + upper)
    solved = state - product(parent, pull, ROWS)
    narrow = solved.astype(jnp.bfloat16)
    beside = lax.ppermute(narrow, "leaf", [(k, k + 1) for k in range(0, count, 2)])
    parent_rows = jnp.where(even, narrow, beside)

    parent_full = join(parent_rows, swap(parent_rows), first, 0)
    pulled = jnp.dot(parent_full, couple_cols, preferred_element_type=jnp.float32)
    residue = (leaf_state.astype(jnp.float32) - pulled).astype(jnp.bfloat16)
    away = product(residue, columns(inv_rows, 1 - core, wide), ROWS, None)
    arrived = swap(away)
    here = product(residue, columns(inv_rows, core, wide), ROWS, None)
    leaf_solution = here + arrived

    solved_late, from_below, _ = lax.optimization_barrier((solved, from_below, parent_rows))
    whole = jnp.where(place == top, from_below, solved_late)
    sep_solution = join(
        columns(whole, core, half_sep), swap(columns(whole, 1 - core, half_sep)), first, 0
    )
    return (leaf_solution[None], sep_solution[None])


def solution(mesh):
    return jax.shard_map(
        solve,
        mesh=mesh,
        in_specs=(
            P("leaf", None, "sep"),
            P("leaf", "sep", None),
            P("leaf", None, "sep"),
            P("leaf", None, "sep"),
            P("leaf", "sep", None),
            P("leaf", None, "sep"),
        ),
        out_specs=(P("leaf", None, "sep"), P("leaf", None, "sep")),
        check_vma=False,
    )
```

```python
import jax
import jax.numpy as jnp
from jax import lax
from jax.sharding import PartitionSpec as P


ROWS = (((1,), (0,)), ((), ()))
BOTH = (((1,), (1,)), ((), ()))
FIRST = (((0,), (0,)), ((), ()))


def product(left, right, dims, precision=lax.Precision.HIGH):
    return lax.dot_general(
        left, right, dims, precision=precision, preferred_element_type=jnp.float32
    )


def swap(value):
    pairs = [(source, source ^ 1) for source in range(lax.axis_size("sep"))]
    return lax.ppermute(value, "sep", pairs)


def send(value, pairs):
    return lax.ppermute(value.astype(jnp.bfloat16), "leaf", pairs).astype(jnp.float32)


def join(mine, other, first, axis):
    return jnp.where(
        first,
        jnp.concatenate([mine, other], axis=axis),
        jnp.concatenate([other, mine], axis=axis),
    )


def columns(value, which, wide):
    return lax.dynamic_slice_in_dim(value, which * wide, wide, 1)


def solve(leaf_rhs, leaf_inv, leaf_couple, sep_rhs, sep_inv, sep_couple):
    count = lax.axis_size("leaf")
    depth = count.bit_length() - 1
    place = lax.axis_index("leaf")
    core = lax.axis_index("sep")
    first = core == 0
    even = place % 2 == 0
    inv_rows = leaf_inv[0]
    couple_cols = leaf_couple[0]
    half = leaf_rhs.shape[1] // 2
    half_sep = sep_rhs.shape[2]
    top, below = count - 1, count // 2 - 1

    def my_rows(value):
        return lax.dynamic_slice_in_dim(value, core * half, half, 0)

    def other_rows(value):
        return lax.dynamic_slice_in_dim(value, (1 - core) * half, half, 0)

    wide = leaf_rhs.shape[2]
    inv_half, couple_half, sep_local = sep_inv[0], sep_couple[0], sep_rhs[0]
    rhs_own = leaf_rhs[0]
    rhs_other = swap(rhs_own)
    top_half = lax.ppermute(inv_half, "leaf", [(top, below)])
    leaf_state = product(join(rhs_own, rhs_other, first, 1), inv_rows, BOTH, None)
    leaf_state = leaf_state.astype(jnp.bfloat16)
    theirs = product(other_rows(leaf_state), couple_cols, BOTH, None)
    ours = product(my_rows(leaf_state), couple_cols, BOTH, None)

    rhs_rows = join(my_rows(sep_local), swap(other_rows(sep_local)), first, 1)

    def both_cores(part):
        return part + swap(part)

    outgoing = ours + swap(theirs)
    pull_part = product(couple_half, inv_half, ROWS)
    pull = both_cores(pull_part)
    work = rhs_rows - jnp.where(even, outgoing, 0.0)
    received = send(outgoing, [(k + 1, k) for k in range(0, count, 2)])
    work = work - received
    for level in range(1, depth):
        reach = 2 ** (level - 1)
        parents = range(2 * reach - 1, count, 4 * reach)
        outgoing = product(work, pull, BOTH)
        lower = send(outgoing, [(k - reach, k) for k in parents])
        upper = send(outgoing, [(k + reach, k) for k in parents])
        if level == 1:
            inv_late, rhs_late, _ = lax.optimization_barrier((inv_half, rhs_rows, outgoing))
            gram = both_cores(product(inv_late, inv_late, FIRST))
            top_rhs = lax.ppermute(rhs_late, "leaf", [(top, below)])
        if level == 2:
            top_late, _ = lax.optimization_barrier((top_half, outgoing))
            top_gram = both_cores(product(top_late, top_late, FIRST))
        work = work - (lower + upper)
    top_work = top_rhs - product(work, pull, BOTH)
    top_solution = product(top_work, top_gram, ROWS)
    parent = top_solution
    state = product(work, gram, ROWS)
    for level in range(depth, 1, -1):
        reach = 2 ** (level - 2)
        slots = range(2 * reach - 1, count, 4 * reach)
        solved = state - product(parent, pull, ROWS)
        lower = send(solved, [(k, k - reach) for k in slots])
        upper = send(solved, [(k, k + reach) for k in slots])
        parent = parent + (lower + upper)
    solved = state - product(parent, pull, ROWS)
    from_below = lax.ppermute(top_solution, "leaf", [(below, top)])
    whole = jnp.where(place == top, from_below, solved)
    narrow = whole.astype(jnp.bfloat16)
    beside = lax.ppermute(narrow, "leaf", [(k, k + 1) for k in range(0, count, 2)])
    parent_rows = jnp.where(even, narrow, beside)

    whole_arrived = swap(columns(whole, 1 - core, half_sep))
    sep_solution = join(columns(whole, core, half_sep), whole_arrived, first, 0)

    parent_full = join(parent_rows, swap(parent_rows), first, 0)
    pulled = jnp.dot(parent_full, couple_cols, preferred_element_type=jnp.float32)
    residue = (leaf_state.astype(jnp.float32) - pulled).astype(jnp.bfloat16)
    away = product(residue, columns(inv_rows, 1 - core, wide), ROWS, None)
    arrived = swap(away)
    here = product(residue, columns(inv_rows, core, wide), ROWS, None)
    leaf_solution = here + arrived

    return (leaf_solution[None], sep_solution[None])


def solution(mesh):
    return jax.shard_map(
        solve,
        mesh=mesh,
        in_specs=(
            P("leaf", None, "sep"),
            P("leaf", "sep", None),
            P("leaf", None, "sep"),
            P("leaf", None, "sep"),
            P("leaf", "sep", None),
            P("leaf", None, "sep"),
        ),
        out_specs=(P("leaf", None, "sep"), P("leaf", None, "sep")),
        check_vma=False,
    )
```

```python
import jax
import jax.numpy as jnp
from jax import lax
from jax.sharding import PartitionSpec as P


ROWS = (((1,), (0,)), ((), ()))
BOTH = (((1,), (1,)), ((), ()))
FIRST = (((0,), (0,)), ((), ()))


def product(left, right, dims, precision=lax.Precision.HIGH):
    return lax.dot_general(
        left, right, dims, precision=precision, preferred_element_type=jnp.float32
    )


def swap(value):
    pairs = [(source, source ^ 1) for source in range(lax.axis_size("sep"))]
    return lax.ppermute(value, "sep", pairs)


def send(value, pairs):
    return lax.ppermute(value.astype(jnp.bfloat16), "leaf", pairs).astype(jnp.float32)


def join(mine, other, first, axis):
    return jnp.where(
        first,
        jnp.concatenate([mine, other], axis=axis),
        jnp.concatenate([other, mine], axis=axis),
    )


def solve(leaf_rhs, leaf_inv, leaf_couple, sep_rhs, sep_inv, sep_couple):
    count = lax.axis_size("leaf")
    depth = count.bit_length() - 1
    place = lax.axis_index("leaf")
    core = lax.axis_index("sep")
    first = core == 0
    even = place % 2 == 0
    inv_rows = leaf_inv[0]
    couple_cols = leaf_couple[0]
    half = leaf_rhs.shape[1] // 2
    half_sep = sep_rhs.shape[2]
    top, below = count - 1, count // 2 - 1

    def my_rows(value):
        return lax.dynamic_slice_in_dim(value, core * half, half, 0)

    def other_rows(value):
        return lax.dynamic_slice_in_dim(value, (1 - core) * half, half, 0)

    inv_half = sep_inv[0]
    rhs_full = join(leaf_rhs[0], swap(leaf_rhs[0]), first, 1)
    top_half = lax.ppermute(inv_half, "leaf", [(top, below)])
    leaf_state = product(rhs_full, inv_rows, BOTH, None).astype(jnp.bfloat16)
    theirs = product(other_rows(leaf_state), couple_cols, BOTH, None)
    ours = product(my_rows(leaf_state), couple_cols, BOTH, None)

    sep_local = sep_rhs[0]
    rhs_rows = join(my_rows(sep_local), swap(other_rows(sep_local)), first, 1)
    inverse = join(inv_half, swap(inv_half), first, 0)
    couple = join(sep_couple[0], swap(sep_couple[0]), first, 1)
    pull = product(couple, inverse, ROWS)
    gram = product(inverse, inverse, FIRST)
    top_rhs = lax.ppermute(rhs_rows, "leaf", [(top, below)])
    top_inverse = join(top_half, swap(top_half), first, 0)
    top_gram = product(top_inverse, top_inverse, FIRST)

    outgoing = ours + swap(theirs)
    work = rhs_rows - jnp.where(even, outgoing, 0.0)
    work = work - send(outgoing, [(k + 1, k) for k in range(0, count, 2)])
    for level in range(1, depth):
        reach = 2 ** (level - 1)
        parents = range(2 * reach - 1, count, 4 * reach)
        outgoing = product(work, pull, BOTH)
        lower = send(outgoing, [(k - reach, k) for k in parents])
        upper = send(outgoing, [(k + reach, k) for k in parents])
        work = work - (lower + upper)
    top_work = top_rhs - product(work, pull, BOTH)
    top_solution = product(top_work, top_gram, ROWS)
    parent = top_solution
    state = product(work, gram, ROWS)
    for level in range(depth, 1, -1):
        reach = 2 ** (level - 2)
        slots = range(2 * reach - 1, count, 4 * reach)
        solved = state - product(parent, pull, ROWS)
        lower = send(solved, [(k, k - reach) for k in slots])
        upper = send(solved, [(k, k + reach) for k in slots])
        parent = parent + (lower + upper)
    solved = state - product(parent, pull, ROWS)
    beside = lax.ppermute(
        solved.astype(jnp.bfloat16), "leaf", [(k, k + 1) for k in range(0, count, 2)]
    )
    parent_rows = jnp.where(even, solved.astype(jnp.bfloat16), beside)

    parent_full = join(parent_rows, swap(parent_rows), first, 0)
    pulled = jnp.dot(parent_full, couple_cols, preferred_element_type=jnp.float32)
    residue = (leaf_state.astype(jnp.float32) - pulled).astype(jnp.bfloat16)
    spread = jnp.dot(residue, inv_rows, preferred_element_type=jnp.float32)
    wide = leaf_rhs.shape[2]
    away = lax.dynamic_slice_in_dim(spread, (1 - core) * wide, wide, 1)
    here = lax.dynamic_slice_in_dim(spread, core * wide, wide, 1)
    leaf_solution = here + swap(away)

    from_below = lax.ppermute(top_solution, "leaf", [(below, top)])
    whole = jnp.where(place == top, from_below, solved)
    away = lax.dynamic_slice_in_dim(whole, (1 - core) * half_sep, half_sep, 1)
    here = lax.dynamic_slice_in_dim(whole, core * half_sep, half_sep, 1)
    sep_solution = join(here, swap(away), first, 0)
    return (leaf_solution[None], sep_solution[None])


def solution(mesh):
    return jax.shard_map(
        solve,
        mesh=mesh,
        in_specs=(
            P("leaf", None, "sep"),
            P("leaf", "sep", None),
            P("leaf", None, "sep"),
            P("leaf", None, "sep"),
            P("leaf", "sep", None),
            P("leaf", None, "sep"),
        ),
        out_specs=(P("leaf", None, "sep"), P("leaf", None, "sep")),
        check_vma=False,
    )
```
